128 devices in a mesh: prow: 8 (over x, core), pcol: 16 (over z, y).
Axes of the slice: x: 4, y: 4, z: 4, core: 2. Of those that a mesh axis runs over, the one named last changes fastest.
Arguments:
- panels: bfloat16 [2, 96, 2048, 256], P(None, 'pcol', 'prow'), may hold values from -0.59765625 to 0.59765625
- inverses: bfloat16 [2, 96, 256, 256], P(None, 'pcol', 'prow'), may hold values from -0.25 to 0.25
- dest: int32 [96, 8, 8], P('pcol', 'prow'), may hold values from 0 to 15, as said below
- target: int32 [96, 8, 8], P('pcol', 'prow'), may hold values from 0 to 1
- ancestors: float32 [2, 4096, 4096], P(None, 'prow', 'pcol'), may hold values from -6 to 6
Outputs:
- factor: bfloat16 [2, 96, 2048, 256], P(None, 'pcol', 'prow')
- schur: float32 [2, 4096, 4096], P(None, 'prow', 'pcol')
The draws below stay inside these ranges and needn't reach their ends.
Inputs may be any that keep to these rules, and one draw needn't show every extreme that they name: `dest`: among the 48 update blocks of one device (its leaves, its block rows), at most 6 name any one process column; on every process row one process column is named by exactly 6 blocks of every device of that row.
All inputs are finite; a program needn't handle non-finite values.
Results may differ from the reference program's by a relative error of at most 0.0045.
Values may be sent and summed in bfloat16 or wider, within the bound.
A program may use at most 128 MiB of HBM per device.

```python
import jax
import jax.numpy as jnp
from jax import lax

W = 256
ROWB = 8
LEAF_DEV = 6
ANC_DEV = 2
CAP = 6
LEAVES = 96
FRONT = 2048
ANC_ROWS = 4096
ANC_COLS = 4096
N_PROW = 8
N_PCOL = 16


def draw_dest(key, part):
    rows_local = ROWB // N_PROW
    block_count = LEAF_DEV * rows_local * ROWB
    row_keys = jax.random.split(jax.random.fold_in(key, 11), N_PROW)

    def per_row(row_key):
        full_dest = jax.random.randint(jax.random.fold_in(row_key, 1), (), 0, N_PCOL).astype(jnp.int32)

        def per_device(device_key):
            others = (full_dest + 1 + jnp.arange((N_PCOL - 1) * CAP, dtype=jnp.int32) // CAP) % N_PCOL
            shuffled = jax.random.permutation(jax.random.fold_in(device_key, 2), others)
            chosen = jnp.concatenate([jnp.full((CAP,), full_dest, jnp.int32), shuffled[:block_count - CAP]])
            return jax.random.permutation(jax.random.fold_in(device_key, 3), chosen)
        return jax.vmap(per_device)(jax.random.split(jax.random.fold_in(row_key, 4), N_PCOL))
    layout = jax.vmap(per_row)(row_keys)
    layout = layout.reshape(N_PROW, N_PCOL, LEAF_DEV, rows_local, ROWB)
    return layout.transpose(1, 2, 0, 3, 4).reshape(LEAF_DEV * N_PCOL, ROWB, ROWB).astype(jnp.int32)


def touch_ends(result, stream_key, low, top_value):
    place = [jax.random.randint(jax.random.fold_in(stream_key, axis), (), 0, length) for axis, length in enumerate(result.shape)]
    longest = result.shape.index(max(result.shape))
    beside = place[:longest] + [(place[longest] + 1) % result.shape[longest]] + place[longest + 1:]
    return result.at[tuple(place)].set(low).at[tuple(beside)].set(top_value)


def block_scale(stream_key, dims, pieces, low, high):
    loudness = 1.0
    for position, blocks in pieces:
        heights = jax.random.uniform(jax.random.fold_in(jax.random.fold_in(stream_key, 6), position), (blocks,), jnp.float32, low / len(pieces), high / len(pieces))
        loudness = loudness * jnp.repeat(jnp.exp(heights), dims[position] // blocks).reshape((-1,) + (1,) * (len(dims) - 1 - position))
    return loudness


def bell_draw(rng, shape, spread, bound, shards=(), kind=jnp.bfloat16):
    values = spread * jax.random.normal(rng, shape, jnp.float32)
    if shards:
        values = values * block_scale(rng, shape, shards, -0.22, 0.18)
    return jnp.clip(values, -bound, bound).astype(kind)


def setup_inputs(seed: int = 0) -> dict:
    keys = jax.random.split(jax.random.key(seed), 6)
    return {
        "panels": bell_draw(keys[0], (2, LEAVES, FRONT, W), 0.1, 0.59765625, ((1, 16), (2, 8))),
        "inverses": bell_draw(keys[1], (2, LEAVES, W, W), (2 * W) ** -0.5, 0.25, ((1, 16), (2, 8))),
        "dest": draw_dest(jax.random.fold_in(keys[5], 71), 0),
        "target": touch_ends(jax.random.randint(keys[3], (LEAVES, ROWB, ROWB), 0, ANC_DEV), jax.random.fold_in(keys[3], 1), 0, ANC_DEV - 1).astype(jnp.int32),
        "ancestors": bell_draw(keys[4], (2, ANC_ROWS, ANC_COLS), 1.0, 6.0, ((1, 8), (2, 16)), jnp.float32),
    }


def complex_dot(left_side, right_side):
    real_part = jnp.dot(left_side[0], right_side[0], preferred_element_type=jnp.float32) - jnp.dot(left_side[1], right_side[1], preferred_element_type=jnp.float32)
    imag_part = jnp.dot(left_side[0], right_side[1], preferred_element_type=jnp.float32) + jnp.dot(left_side[1], right_side[0], preferred_element_type=jnp.float32)
    return jnp.stack([real_part, imag_part])


def reference(panels, inverses, dest, target, ancestors):
    rows_local = ROWB // N_PROW
    block_rows = jnp.arange(ROWB, dtype=jnp.int32)[:, None] // rows_local

    def per_leaf(totals, inputs):
        panel, inverse, leaf_dest, leaf_target = inputs
        lower_panel = complex_dot(panel, inverse).astype(jnp.bfloat16)
        update = complex_dot(lower_panel, jnp.swapaxes(panel, 1, 2)).astype(jnp.bfloat16)
        update = lax.optimization_barrier(update).astype(jnp.float32)
        blocks = update.reshape(2, ROWB, W, ROWB, W).transpose(1, 3, 0, 2, 4).reshape(ROWB * ROWB, 2, W, W)
        index = ((block_rows * ANC_DEV + leaf_target) * N_PCOL + leaf_dest).reshape(-1).astype(jnp.int32)
        return totals.at[index].add(blocks), lower_panel

    initial = jnp.zeros((N_PROW * ANC_DEV * N_PCOL, 2, W, W), jnp.float32)
    totals, lowers = lax.scan(per_leaf, initial, (panels.transpose(1, 0, 2, 3), inverses.transpose(1, 0, 2, 3), dest, target))
    factor = lowers.transpose(1, 0, 2, 3)
    layout = totals.reshape(N_PROW, ANC_DEV, N_PCOL, 2, W, W).transpose(3, 0, 1, 4, 2, 5)
    layout = layout.reshape(2, N_PROW * ANC_DEV * W, N_PCOL * W)
    return factor, ancestors - layout
```

```python
import functools

import jax
import jax.numpy as jnp
from jax import lax
from jax.experimental import pallas as pl
from jax.experimental.pallas import tpu as pltpu
from jax.sharding import PartitionSpec as P

MESH = pl.DeviceIdType.MESH
CHUNKS = 8
RING = 4
CAP = 6


def dot(a, b):
    return jnp.dot(a, b, preferred_element_type=jnp.float32)


def dot_t(a, b):
    return lax.dot_general(a, b, (((1,), (1,)), ((), ())), preferred_element_type=jnp.float32)


def kernel(
    table, panels, inverses, factor, summed,
    pan, inv, fac, upd, mer, t1, g1, t2, g2, res,
    psend, precv, isend, irecv, rsend, rrecv, load, store,
):
    n_chunks, _, leaves, rows_b, h, width = pan.shape
    part = inverses.shape[2]
    px, pc = lax.axis_index("prow"), lax.axis_index("pcol")
    x, core = px // 2, px % 2
    z, y = pc // RING, pc % RING

    def at_x(step, other=0):
        return ((x + step) % RING) * 2 + (core if not other else 1 - core)

    def at_yz(dy, dz):
        return ((z + dz) % RING) * RING + (y + dy) % RING

    x_next, x_prev, mate = (at_x(1), pc), (at_x(3), pc), (at_x(0, 1), pc)
    y_next, y_prev = (px, at_yz(1, 0)), (px, at_yz(3, 0))
    z_next, z_prev = (px, at_yz(0, 1)), (px, at_yz(0, 3))

    def remote(src, dst, send, recv, device):
        return pltpu.make_async_remote_copy(
            src_ref=src, dst_ref=dst, send_sem=send, recv_sem=recv,
            device_id=device, device_id_type=MESH,
        )

    def gather_copy(view, send, recv, n):
        blocks = (px, px, px, at_x(3), at_x(1), at_x(3), at_x(1), at_x(2), at_x(2))
        planes = (None, None, None, 0, 1, None, None, 0, 1)
        devices = (x_next, x_prev, mate, x_next, x_prev, mate, mate, mate, mate)
        src = view(blocks[n], planes[n])
        return remote(src, src, send(n), recv(n), devices[n])

    def gather_wait(view, send, recv, n):
        blocks = (
            at_x(3), at_x(1), at_x(0, 1), at_x(2), at_x(2),
            at_x(3, 1), at_x(1, 1), at_x(2, 1), at_x(2, 1),
        )
        planes = (None, None, None, 0, 1, None, None, 0, 1)
        dst = view(blocks[n], planes[n])
        remote(dst, dst, send(n), recv(n), mate).wait_recv()

    def pan_args(k):
        def view(block, plane):
            return pan.at[k, :, :, block] if plane is None else pan.at[k, plane, :, block]

        return view, (lambda n: psend.at[k, n]), (lambda n: precv.at[k, n])

    def inv_view(block, plane):
        rows = pl.ds(pl.multiple_of(block * part, part), part)
        return inv.at[:, :, rows] if plane is None else inv.at[plane, :, rows]

    inv_args = (inv_view, (lambda n: isend.at[n]), (lambda n: irecv.at[n]))

    def sum_copy(k, half, n):
        first_next, first_prev = (y_next, y_prev) if half == 0 else (z_next, z_prev)
        then_next, then_prev = (z_next, z_prev) if half == 0 else (y_next, y_prev)
        m, t, g = mer.at[k, half], t1.at[k, half], g1.at[k, half]
        tt, gg = t2.at[k, half], g2.at[k, half]
        src, dst, device = (
            (m.at[2, 0:2], t.at[0], first_next),
            (m.at[2, 2:4], t.at[1], first_prev),
            (m.at[1, 2:4], g.at[0, 2:4], first_next),
            (m.at[3, 0:2], g.at[1, 0:2], first_prev),
            (m.at[1, 0:2], g.at[0, 0:2], first_next),
            (m.at[3, 2:4], g.at[1, 2:4], first_prev),
            (m.at[0, 2, 0], tt.at[0], then_next),
            (m.at[0, 2, 1], tt.at[1], then_prev),
            (m.at[0, 1, 1], gg.at[0, 1], then_next),
            (m.at[0, 3, 0], gg.at[1, 0], then_prev),
            (m.at[0, 1, 0], gg.at[0, 0], then_next),
            (m.at[0, 3, 1], gg.at[1, 1], then_prev),
        )[n]
        return remote(src, dst, rsend.at[k, half * 12 + n], rrecv.at[k, half * 12 + n], device)

    def load_pan(k):
        rows = pl.ds(pl.multiple_of(k * h, h), h)
        return pltpu.make_async_copy(panels.at[:, :, rows], pan.at[k, :, :, px], load.at[k])

    load_inv = pltpu.make_async_copy(inverses, inv_view(px, None), load.at[n_chunks])
    store_factor = pltpu.make_async_copy(fac.at[0:2], factor, store.at[n_chunks])

    def store_sum(k):
        rows = pl.ds(pl.multiple_of(k * h, h), h)
        return pltpu.make_async_copy(res.at[k], summed.at[:, :, rows], store.at[k])

    load_inv.start()
    for k in range(n_chunks):
        load_pan(k).start()

    barrier = pltpu.get_barrier_semaphore()
    neighbours = (x_next, x_prev, mate, y_next, y_prev, z_next, z_prev)
    for device in neighbours:
        pl.semaphore_signal(barrier, inc=1, device_id=device, device_id_type=MESH)
    upd[upd.shape[0] - 1] = jnp.zeros(upd.shape[1:], upd.dtype)
    pl.semaphore_wait(barrier, len(neighbours))

    load_inv.wait()
    for n in (0, 1, 2):
        gather_copy(*inv_args, n).start()
    for k in range(n_chunks):
        load_pan(k).wait()
    for n in (0, 1, 2):
        gather_copy(*pan_args(0), n).start()
    for n in (0, 1):
        gather_wait(*inv_args, n)
    for n in (3, 4, 5, 6):
        gather_copy(*inv_args, n).start()
    for n in (0, 1, 2):
        gather_copy(*pan_args(1), n).start()

    def in_turn(k, stage):
        @pl.when(jnp.logical_and(k >= 0, k < n_chunks))
        def _():
            stage(k)

    def relay_first(k):
        for n in (0, 1):
            gather_wait(*pan_args(k), n)
        for n in (3, 4, 5, 6):
            gather_copy(*pan_args(k), n).start()

        @pl.when(k + 2 < n_chunks)
        def _():
            for n in (0, 1, 2):
                gather_copy(*pan_args(k + 2), n).start()

    def relay_second(k):
        for n in (3, 4):
            gather_wait(*pan_args(k), n)
        for n in (7, 8):
            gather_copy(*pan_args(k), n).start()

    def make_factor():
        for n in (3, 4):
            gather_wait(*inv_args, n)
        for n in (7, 8):
            gather_copy(*inv_args, n).start()
        for n in (2, 5, 6, 7, 8):
            gather_wait(*inv_args, n)

        def leaf(s, carry):
            real = pan[:, 0, s, px].reshape(width, width)
            imag = pan[:, 1, s, px].reshape(width, width)
            inv_real, inv_imag = inv[0, s], inv[1, s]
            fac[0, s] = (dot(real, inv_real) - dot(imag, inv_imag)).astype(fac.dtype)
            turned = dot(real, inv_imag) + dot(imag, inv_real)
            fac[1, s] = turned.astype(fac.dtype)
            fac[2, s] = (-turned).astype(fac.dtype)
            return carry

        lax.fori_loop(0, leaves, leaf, 0)
        store_factor.start()

    def multiply(k):
        for n in (2, 5, 6, 7, 8):
            gather_wait(*pan_args(k), n)

        def leaf(s, carry):
            real = pan[k, 0, s].reshape(rows_b * h, width)
            imag = pan[k, 1, s].reshape(rows_b * h, width)
            first = pl.multiple_of(s * rows_b, rows_b)
            product = dot_t(real, fac[0, s]) + dot_t(imag, fac[2, s])
            upd[pl.ds(first, rows_b), 0] = product.astype(upd.dtype).reshape(rows_b, h, width)
            product = dot_t(real, fac[1, s]) + dot_t(imag, fac[0, s])
            upd[pl.ds(first, rows_b), 1] = product.astype(upd.dtype).reshape(rows_b, h, width)
            return carry

        lax.fori_loop(0, leaves, leaf, 0)

        def merge(q, carry):
            half, f, g = q // 16, (q // 4) % 4, q % 4
            owner = at_yz(f + half * (g - f), g + half * (f - g))
            entry = (owner * 2 + half) * CAP
            total = upd[table[entry]].astype(jnp.float32)
            for i in range(1, CAP):
                total += upd[table[entry + i]].astype(jnp.float32)
            mer[k, half, f, g] = total.astype(mer.dtype)
            return carry

        lax.fori_loop(0, 32, merge, 0)
        for n in (0, 1, 2, 3):
            for half in (0, 1):
                sum_copy(k, half, n).start()

    def add_to(ref, other):
        ref[...] = (ref[...].astype(jnp.float32) + other[...].astype(jnp.float32)).astype(ref.dtype)

    def sum_b(k):
        for half in (0, 1):
            for n in (0, 1):
                sum_copy(k, half, n).wait_recv()
            add_to(mer.at[k, half, 1, 0:2], t1.at[k, half, 0])
            add_to(mer.at[k, half, 3, 2:4], t1.at[k, half, 1])
        for half in (0, 1):
            for n in (4, 5):
                sum_copy(k, half, n).start()

    def sum_c(k):
        for half in (0, 1):
            for n in (2, 3, 4, 5):
                sum_copy(k, half, n).wait_recv()
            total = mer[k, half, 0].astype(jnp.float32)
            total += g1[k, half, 0].astype(jnp.float32)
            total += g1[k, half, 1].astype(jnp.float32)
            mer[k, half, 0] = total.astype(mer.dtype)
        for n in (6, 7, 8, 9):
            for half in (0, 1):
                sum_copy(k, half, n).start()

    def sum_d(k):
        for half in (0, 1):
            for n in (6, 7):
                sum_copy(k, half, n).wait_recv()
            add_to(mer.at[k, half, 0, 1, 0], t2.at[k, half, 0])
            add_to(mer.at[k, half, 0, 3, 1], t2.at[k, half, 1])
        for half in (0, 1):
            for n in (10, 11):
                sum_copy(k, half, n).start()

    def sum_e(k):
        for half in (0, 1):
            for n in (8, 9, 10, 11):
                sum_copy(k, half, n).wait_recv()
            total = mer[k, half, 0, 0].astype(jnp.float32)
            total += g2[k, half, 0].astype(jnp.float32)
            total += g2[k, half, 1].astype(jnp.float32)
            res[k, half] = total
        store_sum(k).start()

    def step(i, carry):
        in_turn(i, relay_first)
        in_turn(i - 1, relay_second)
        pl.when(i == 1)(make_factor)
        in_turn(i - 6, sum_e)
        in_turn(i - 5, sum_d)
        in_turn(i - 4, sum_c)
        in_turn(i - 3, sum_b)
        in_turn(i - 2, multiply)
        return carry

    lax.fori_loop(0, n_chunks + 7, step, 0)

    for n in range(9):
        gather_copy(*inv_args, n).wait_send()

    def drain(k, carry):
        for n in range(9):
            gather_copy(*pan_args(k), n).wait_send()
        for half in (0, 1):
            for n in range(12):
                sum_copy(k, half, n).wait_send()
        store_sum(k).wait()
        return carry

    lax.fori_loop(0, n_chunks, drain, 0)
    store_factor.wait()


def local(panels, inverses, dest, target, ancestors):
    _, leaves, rows, width = panels.shape
    rows_b = dest.shape[2]
    h = rows // CHUNKS
    blocks = leaves * rows_b
    slots = RING * RING * 2
    keys = (dest * 2 + target).reshape(-1)
    order = jnp.arange(blocks, dtype=jnp.int32)
    same = (keys[:, None] == keys[None, :]) & (order[None, :] < order[:, None])
    rank = jnp.sum(same.astype(jnp.int32), axis=1)
    place = keys * CAP + rank
    hit = jnp.arange(slots * CAP, dtype=jnp.int32)[:, None] == place[None, :]
    table = jnp.min(jnp.where(hit, order[None, :], blocks), axis=1).astype(jnp.int32)

    bf16, f32 = jnp.bfloat16, jnp.float32
    any_space = pl.BlockSpec(memory_space=pl.ANY)
    dma = pltpu.SemaphoreType.DMA
    factor, summed = pl.pallas_call(
        kernel,
        out_shape=(
            jax.ShapeDtypeStruct(panels.shape, bf16),
            jax.ShapeDtypeStruct((2, 2, rows, width), f32),
        ),
        in_specs=[pl.BlockSpec(memory_space=pltpu.SMEM), any_space, any_space],
        out_specs=(any_space, any_space),
        scratch_shapes=[
            pltpu.VMEM((CHUNKS, 2, leaves, rows_b, h, width), bf16),
            pltpu.VMEM((2, leaves, width, width), bf16),
            pltpu.VMEM((3, leaves, rows, width), bf16),
            pltpu.VMEM((blocks + 1, 2, h, width), bf16),
            pltpu.VMEM((CHUNKS, 2, 4, 4, 2, h, width), bf16),
            pltpu.VMEM((CHUNKS, 2, 2, 2, 2, h, width), bf16),
            pltpu.VMEM((CHUNKS, 2, 2, 4, 2, h, width), bf16),
            pltpu.VMEM((CHUNKS, 2, 2, h, width), bf16),
            pltpu.VMEM((CHUNKS, 2, 2, 2, h, width), bf16),
            pltpu.VMEM((CHUNKS, 2, 2, h, width), f32),
            dma((CHUNKS, 9)), dma((CHUNKS, 9)), dma((9,)), dma((9,)),
            dma((CHUNKS, 24)), dma((CHUNKS, 24)), dma((CHUNKS + 1,)), dma((CHUNKS + 1,)),
        ],
        compiler_params=pltpu.CompilerParams(
            collective_id=0, has_side_effects=True, vmem_limit_bytes=60 * 1024 * 1024
        ),
    )(table, panels, inverses)
    summed = summed.transpose(1, 0, 3, 2).reshape(ancestors.shape)
    return factor, ancestors - summed


def solution(mesh):
    return jax.shard_map(
        local,
        mesh=mesh,
        in_specs=(
            P(None, "pcol", "prow", None),
            P(None, "pcol", "prow", None),
            P("pcol", "prow", None),
            P("pcol", "prow", None),
            P(None, "prow", "pcol"),
        ),
        out_specs=(P(None, "pcol", "prow", None), P(None, "prow", "pcol")),
        check_vma=False,
    )
```

```python
import functools

import jax
import jax.numpy as jnp
from jax import lax
from jax.experimental import pallas as pl
from jax.experimental.pallas import tpu as pltpu
from jax.sharding import PartitionSpec as P

MESH = pl.DeviceIdType.MESH
CHUNKS = 8
RING = 4
CAP = 6
LAG2, LAGM, LAG, AHEAD = 1, 1, 1, 2
ORDER = "12ecbm"


def dot(a, b):
    return jnp.dot(a, b, preferred_element_type=jnp.float32)


def dot_t(a, b):
    return lax.dot_general(a, b, (((1,), (1,)), ((), ())), preferred_element_type=jnp.float32)


def kernel(
    dest, target, panels, inverses, factor, summed,
    keys, table, pan, inv, minus, upd, mer, t1, g1, g2,
    psend, precv, isend, irecv, rsend, rrecv, load,
):
    n_chunks, _, leaves, rows_b, h, width = pan.shape
    part = inverses.shape[2]
    px, pc = lax.axis_index("prow"), lax.axis_index("pcol")
    x, core = px // 2, px % 2
    z, y = pc // RING, pc % RING

    def at_x(step, other=0):
        return ((x + step) % RING) * 2 + (core if not other else 1 - core)

    def at_yz(dy, dz):
        return ((z + dz) % RING) * RING + (y + dy) % RING

    x_next, x_prev, mate = (at_x(1), pc), (at_x(3), pc), (at_x(0, 1), pc)
    y_next, y_prev = (px, at_yz(1, 0)), (px, at_yz(3, 0))
    z_next, z_prev = (px, at_yz(0, 1)), (px, at_yz(0, 3))
    y_far, z_far = (px, at_yz(2, 0)), (px, at_yz(0, 2))

    def remote(src, dst, send, recv, device):
        return pltpu.make_async_remote_copy(
            src_ref=src, dst_ref=dst, send_sem=send, recv_sem=recv,
            device_id=device, device_id_type=MESH,
        )

    def gather_copy(view, send, recv, n):
        blocks = (px, px, px, at_x(3), at_x(1), at_x(3), at_x(1), at_x(2), at_x(2))
        planes = (None, None, None, 0, 1, None, None, 0, 1)
        devices = (x_next, x_prev, mate, x_next, x_prev, mate, mate, mate, mate)
        src = view(blocks[n], planes[n])
        return remote(src, src, send(n), recv(n), devices[n])

    def gather_wait(view, send, recv, n):
        blocks = (
            at_x(3), at_x(1), at_x(0, 1), at_x(2), at_x(2),
            at_x(3, 1), at_x(1, 1), at_x(2, 1), at_x(2, 1),
        )
        planes = (None, None, None, 0, 1, None, None, 0, 1)
        dst = view(blocks[n], planes[n])
        remote(dst, dst, send(n), recv(n), mate).wait_recv()

    def pan_args(k):
        def view(block, plane):
            return pan.at[k, :, :, block] if plane is None else pan.at[k, plane, :, block]

        return view, (lambda n: psend.at[k, n]), (lambda n: precv.at[k, n])

    def inv_view(block, plane):
        rows = pl.ds(pl.multiple_of(block * part, part), part)
        return inv.at[:, :, rows] if plane is None else inv.at[plane, :, rows]

    inv_args = (inv_view, (lambda n: isend.at[n]), (lambda n: irecv.at[n]))

    def sum_copy(k, half, n):
        along_y, along_z = (y_next, y_prev, y_far), (z_next, z_prev, z_far)
        first, then = (along_y, along_z) if half == 0 else (along_z, along_y)
        m, t, g, gg = mer.at[k, half], t1.at[k, half], g1.at[k, half], g2.at[k, half]
        src, dst, device = (
            (m.at[2, 0:2], t.at[0], first[0]),
            (m.at[2, 2:4], t.at[1], first[1]),
            (m.at[1, 2:4], g.at[0, 2:4], first[0]),
            (m.at[3, 0:2], g.at[1, 0:2], first[1]),
            (m.at[1, 0:2], g.at[0, 0:2], first[0]),
            (m.at[3, 2:4], g.at[1, 2:4], first[1]),
            (m.at[0, 2], gg.at[2], then[2]),
            (m.at[0, 1], gg.at[0], then[0]),
            (m.at[0, 3], gg.at[1], then[1]),
        )[n]
        return remote(src, dst, rsend.at[k, half * 9 + n], rrecv.at[k, half * 9 + n], device)

    def load_pan(k):
        rows = pl.ds(pl.multiple_of(k * h, h), h)
        return pltpu.make_async_copy(panels.at[:, :, rows], pan.at[k, :, :, px], load.at[k])

    def make_table():
        blocks = leaves * rows_b
        for s in range(leaves):
            for b in range(rows_b):
                keys[s * rows_b + b] = dest[s, 0, b] * 2 + target[s, 0, b]

        def slot(q, carry):
            entries = [jnp.int32(blocks)] * CAP
            for block in range(blocks):
                match = keys[block] == q
                moved = [jnp.int32(block)] + entries[:-1]
                entries = [jnp.where(match, new, old) for new, old in zip(moved, entries)]
            for i in range(CAP):
                table[q * CAP + i] = entries[i]
            return carry

        lax.fori_loop(0, 2 * RING * RING, slot, 0)

    load_inv = pltpu.make_async_copy(inverses, inv_view(px, None), load.at[n_chunks])
    load_inv.start()
    for k in range(n_chunks):
        load_pan(k).start()

    barrier = pltpu.get_barrier_semaphore()
    neighbours = (x_next, x_prev, mate, y_next, y_prev, y_far, z_next, z_prev, z_far)
    for device in neighbours:
        pl.semaphore_signal(barrier, inc=1, device_id=device, device_id_type=MESH)
    upd[upd.shape[0] - 1] = jnp.zeros(upd.shape[1:], upd.dtype)
    pl.semaphore_wait(barrier, len(neighbours))

    load_inv.wait()
    for n in (0, 1, 2):
        gather_copy(*inv_args, n).start()
    for k in range(n_chunks):
        load_pan(k).wait()
    for n in (0, 1, 2):
        gather_copy(*pan_args(0), n).start()
    make_table()
    for n in (0, 1):
        gather_wait(*inv_args, n)
    for n in (3, 4, 5, 6):
        gather_copy(*inv_args, n).start()

    def in_turn(k, first, stage):
        @pl.when(jnp.logical_and(k >= first, k < n_chunks))
        def _():
            stage(k)

    def relay_first(k):
        for n in (0, 1):
            gather_wait(*pan_args(k), n)
        for n in (3, 4, 5, 6):
            gather_copy(*pan_args(k), n).start()

        if isinstance(k, int):
            for later in range(k + 1, k + 1 + AHEAD):
                for n in (0, 1, 2):
                    gather_copy(*pan_args(later), n).start()
            return

        @pl.when(k + AHEAD < n_chunks)
        def _():
            for n in (0, 1, 2):
                gather_copy(*pan_args(k + AHEAD), n).start()

    def relay_second(k):
        for n in (3, 4):
            gather_wait(*pan_args(k), n)
        for n in (7, 8):
            gather_copy(*pan_args(k), n).start()

    def relay_inverses():
        for n in (3, 4):
            gather_wait(*inv_args, n)
        for n in (7, 8):
            gather_copy(*inv_args, n).start()

    def make_factor():
        for n in (2, 5, 6, 7, 8):
            gather_wait(*inv_args, n)

        def leaf(s, carry):
            real = pan[:, 0, s, px].reshape(width, width)
            imag = pan[:, 1, s, px].reshape(width, width)
            inv_real, inv_imag = inv[0, s], inv[1, s]
            factor[0, s] = (dot(real, inv_real) - dot(imag, inv_imag)).astype(factor.dtype)
            turned = dot(real, inv_imag) + dot(imag, inv_real)
            factor[1, s] = turned.astype(factor.dtype)
            minus[s] = (-turned).astype(minus.dtype)
            return carry

        lax.fori_loop(0, leaves, leaf, 0)

    def multiply(k):
        for n in (2, 5, 6, 7, 8):
            gather_wait(*pan_args(k), n)

        def leaf(s, carry):
            real = pan[k, 0, s].reshape(rows_b * h, width)
            imag = pan[k, 1, s].reshape(rows_b * h, width)
            first = pl.multiple_of(s * rows_b, rows_b)
            product = dot_t(real, factor[0, s]) + dot_t(imag, minus[s])
            upd[pl.ds(first, rows_b), 0] = product.astype(upd.dtype).reshape(rows_b, h, width)
            product = dot_t(real, factor[1, s]) + dot_t(imag, factor[0, s])
            upd[pl.ds(first, rows_b), 1] = product.astype(upd.dtype).reshape(rows_b, h, width)
            return carry

        lax.fori_loop(0, leaves, leaf, 0, unroll=leaves)

        def merge(q, carry):
            half, f, g = q // 16, (q // 4) % 4, q % 4
            owner = at_yz(f + half * (g - f), g + half * (f - g))
            entry = (owner * 2 + half) * CAP
            total = upd[table[entry]].astype(jnp.float32)
            for i in range(1, CAP):
                total += upd[table[entry + i]].astype(jnp.float32)
            mer[k, half, f, g] = total.astype(mer.dtype)
            return carry

        lax.fori_loop(0, 32, merge, 0, unroll=2)
        for n in (0, 1, 2, 3):
            for half in (0, 1):
                sum_copy(k, half, n).start()

    def add_to(ref, other):
        ref[...] = (ref[...].astype(jnp.float32) + other[...].astype(jnp.float32)).astype(ref.dtype)

    def sum_b(k):
        for half in (0, 1):
            for n in (0, 1):
                sum_copy(k, half, n).wait_recv()
            add_to(mer.at[k, half, 1, 0:2], t1.at[k, half, 0])
            add_to(mer.at[k, half, 3, 2:4], t1.at[k, half, 1])
        for half in (0, 1):
            for n in (4, 5):
                sum_copy(k, half, n).start()

    def sum_c(k):
        for half in (0, 1):
            for n in (2, 3, 4, 5):
                sum_copy(k, half, n).wait_recv()
            total = mer[k, half, 0].astype(jnp.float32)
            total += g1[k, half, 0].astype(jnp.float32)
            total += g1[k, half, 1].astype(jnp.float32)
            mer[k, half, 0] = total.astype(mer.dtype)
        for n in (6, 7, 8):
            for half in (0, 1):
                sum_copy(k, half, n).start()

    def sum_e(k):
        for half in (0, 1):
            for n in (6, 7, 8):
                sum_copy(k, half, n).wait_recv()
            total = mer[k, half, 0, 0].astype(jnp.float32)
            for n in range(3):
                total += g2[k, half, n].astype(jnp.float32)
            rows = pl.ds(pl.multiple_of(k * h, h), h)
            summed[half, :, rows] = total
        for n in range(9):
            gather_copy(*pan_args(k), n).wait_send()
            for half in (0, 1):
                sum_copy(k, half, n).wait_send()

    relay_first(0)
    relay_inverses()
    relay_second(0)
    make_factor()
    multiply(0)

    stages = {
        "1": (0, 1, relay_first), "2": (LAG2, 1, relay_second), "m": (LAGM, 1, multiply),
        "b": (LAGM + LAG, 0, sum_b), "c": (LAGM + 2 * LAG, 0, sum_c),
        "e": (LAGM + 3 * LAG, 0, sum_e),
    }

    def step(i, carry):
        for name in ORDER:
            lag, first, stage = stages[name]
            in_turn(i - lag, first, stage)
        return carry

    lax.fori_loop(1, n_chunks + LAGM + 3 * LAG, step, 0)

    for n in range(9):
        gather_copy(*inv_args, n).wait_send()


def finish(factor, summed, ancestors, factor_out, schur, res, out, fac_out):
    rows = summed.shape[2]
    keep = [
        pltpu.make_async_copy(factor.at[n], factor_out.at[n], fac_out.at[n]) for n in (0, 1)
    ]
    for one in keep:
        one.start()
    for t in (0, 1):
        for plane in (0, 1):
            here = pl.ds(t * rows, rows)
            res[plane, here] = ancestors[plane, here] - summed[t, plane].T
            store = pltpu.make_async_copy(
                res.at[plane, here], schur.at[plane, here], out.at[t, plane]
            )
            store.start()
            keep.append(store)
    for one in keep:
        one.wait()


def local(panels, inverses, dest, target, ancestors):
    panels = pltpu.with_memory_space_constraint(panels, pltpu.HBM)
    inverses = pltpu.with_memory_space_constraint(inverses, pltpu.HBM)
    _, leaves, rows, width = panels.shape
    rows_b = dest.shape[2]
    h = rows // CHUNKS
    blocks = leaves * rows_b
    bf16, f32 = jnp.bfloat16, jnp.float32
    any_space = pl.BlockSpec(memory_space=pl.ANY)
    vmem = pl.BlockSpec(memory_space=pltpu.VMEM)
    smem = pl.BlockSpec(memory_space=pltpu.SMEM)
    hbm = pl.BlockSpec(memory_space=pltpu.HBM)
    dma = pltpu.SemaphoreType.DMA
    factor, summed = pl.pallas_call(
        kernel,
        out_shape=(
            jax.ShapeDtypeStruct(panels.shape, bf16),
            jax.ShapeDtypeStruct((2, 2, rows, width), f32),
        ),
        in_specs=[smem, smem, hbm, hbm],
        out_specs=(vmem, vmem),
        scratch_shapes=[
            pltpu.SMEM((blocks,), jnp.int32),
            pltpu.SMEM((2 * RING * RING * CAP,), jnp.int32),
            pltpu.VMEM((CHUNKS, 2, leaves, rows_b, h, width), bf16),
            pltpu.VMEM((2, leaves, width, width), bf16),
            pltpu.VMEM((leaves, rows, width), bf16),
            pltpu.VMEM((blocks + 1, 2, h, width), bf16),
            pltpu.VMEM((CHUNKS, 2, 4, 4, 2, h, width), bf16),
            pltpu.VMEM((CHUNKS, 2, 2, 2, 2, h, width), bf16),
            pltpu.VMEM((CHUNKS, 2, 2, 4, 2, h, width), bf16),
            pltpu.VMEM((CHUNKS, 2, 3, 2, h, width), bf16),
            dma((CHUNKS, 9)), dma((CHUNKS, 9)), dma((9,)), dma((9,)),
            dma((CHUNKS, 18)), dma((CHUNKS, 18)), dma((CHUNKS + 1,)),
        ],
        compiler_params=pltpu.CompilerParams(
            collective_id=0, has_side_effects=True, vmem_limit_bytes=40 * 1024 * 1024
        ),
    )(dest, target, panels, inverses)
    return pl.pallas_call(
        finish,
        out_shape=(
            jax.ShapeDtypeStruct(panels.shape, bf16),
            jax.ShapeDtypeStruct(ancestors.shape, f32),
        ),
        in_specs=[vmem, vmem, vmem],
        out_specs=(any_space, any_space),
        scratch_shapes=[pltpu.VMEM(ancestors.shape, f32), dma((2, 2)), dma((2,))],
        compiler_params=pltpu.CompilerParams(vmem_limit_bytes=8 * 1024 * 1024),
    )(factor, summed, ancestors)


def solution(mesh):
    return jax.shard_map(
        local,
        mesh=mesh,
        in_specs=(
            P(None, "pcol", "prow", None),
            P(None, "pcol", "prow", None),
            P("pcol", "prow", None),
            P("pcol", "prow", None),
            P(None, "prow", "pcol"),
        ),
        out_specs=(P(None, "pcol", "prow", None), P(None, "prow", "pcol")),
        check_vma=False,
    )
```

```python
import functools

import jax
import jax.numpy as jnp
from jax import lax
from jax.experimental import pallas as pl
from jax.experimental.pallas import tpu as pltpu
from jax.sharding import PartitionSpec as P

MESH = pl.DeviceIdType.MESH
CHUNKS = 8
RING = 4
CAP = 6
AHEAD = 2
LOOP = (("1", 0), ("e", 4), ("c", 3), ("2", 1), ("b", 2), ("m", 1))
UNROLL = 4
WAITED = (0, 0, 2, 1, 1, 2, 2, 2, 2)


def dot(a, b):
    return jnp.dot(a, b, preferred_element_type=jnp.float32)


def dot_t(a, b):
    return lax.dot_general(a, b, (((1,), (1,)), ((), ())), preferred_element_type=jnp.float32)


def kernel(
    dest, target, panels, inverses, factor, summed,
    dests, targets, keys, table, pan, inv, minus, upd, mer, t1, g1, g2,
    psend, precv, isend, irecv, rsend, rrecv, load,
):
    n_chunks, _, leaves, rows_b, h, width = pan.shape
    part = inverses.shape[2]
    px, pc = lax.axis_index("prow"), lax.axis_index("pcol")
    x, core = px // 2, px % 2
    z, y = pc // RING, pc % RING

    def at_x(step, other=0):
        return ((x + step) % RING) * 2 + (core if not other else 1 - core)

    def at_yz(dy, dz):
        return ((z + dz) % RING) * RING + (y + dy) % RING

    x_next, x_prev, mate = (at_x(1), pc), (at_x(3), pc), (at_x(0, 1), pc)
    y_next, y_prev = (px, at_yz(1, 0)), (px, at_yz(3, 0))
    z_next, z_prev = (px, at_yz(0, 1)), (px, at_yz(0, 3))
    y_far, z_far = (px, at_yz(2, 0)), (px, at_yz(0, 2))

    def remote(src, dst, send, recv, device):
        return pltpu.make_async_remote_copy(
            src_ref=src, dst_ref=dst, send_sem=send, recv_sem=recv,
            device_id=device, device_id_type=MESH,
        )

    def gather_copy(view, send, recv, n):
        blocks = (px, px, px, at_x(3), at_x(1), at_x(3), at_x(1), at_x(2), at_x(2))
        planes = (None, None, None, 0, 1, None, None, 0, 1)
        devices = (x_next, x_prev, mate, x_next, x_prev, mate, mate, mate, mate)
        src = view(blocks[n], planes[n])
        return remote(src, src, send, recv.at[WAITED[n]], devices[n])

    def gather_wait(view, send, recv, group):
        part_of = view(0, None, (2, 1, 4)[group])
        remote(part_of, part_of, send, recv.at[group], mate).wait_recv()

    def gather_drain(view, send, recv):
        part_of = view(0, None, 7)
        remote(part_of, part_of, send, recv.at[0], mate).wait_send()

    def pan_args(k):
        def view(block, plane, count=None):
            if count:
                return pan.at[k, :, :, 0:count]
            return pan.at[k, :, :, block] if plane is None else pan.at[k, plane, :, block]

        return view, psend.at[k], precv.at[k]

    def inv_view(block, plane, count=None):
        if count:
            return inv.at[:, :, 0 : count * part]
        rows = pl.ds(pl.multiple_of(block * part, part), part)
        return inv.at[:, :, rows] if plane is None else inv.at[plane, :, rows]

    inv_args = (inv_view, isend.at[0], irecv)

    def sum_copy(k, half, n):
        along_y, along_z = (y_next, y_prev, y_far), (z_next, z_prev, z_far)
        first, then = (along_y, along_z) if half == 0 else (along_z, along_y)
        m, t, g, gg = mer.at[k, half], t1.at[k, half], g1.at[k, half], g2.at[k, half]
        src, dst, device = (
            (m.at[2, 0:2], t.at[0], first[0]),
            (m.at[2, 2:4], t.at[1], first[1]),
            (m.at[1, 2:4], g.at[0, 2:4], first[0]),
            (m.at[3, 0:2], g.at[1, 0:2], first[1]),
            (m.at[1, 0:2], g.at[0, 0:2], first[0]),
            (m.at[3, 2:4], g.at[1, 2:4], first[1]),
            (m.at[0, 2], gg.at[2], then[2]),
            (m.at[0, 1], gg.at[0], then[0]),
            (m.at[0, 3], gg.at[1], then[1]),
        )[n]
        return remote(src, dst, rsend.at[k], rrecv.at[k, (0, 0, 1, 1, 1, 1, 2, 2, 2)[n]], device)

    def sum_wait(k, group):
        part_of = upd.at[0 : (8, 16, 6)[group]]
        remote(part_of, part_of, rsend.at[k], rrecv.at[k, group], mate).wait_recv()

    def sum_drain(k):
        part_of = upd.at[0:30]
        remote(part_of, part_of, rsend.at[k], rrecv.at[k, 0], mate).wait_send()

    def load_pan(k):
        rows = pl.ds(pl.multiple_of(k * h, h), h)
        return pltpu.make_async_copy(panels.at[:, :, rows], pan.at[k, :, :, px], load.at[0])

    def make_table():
        blocks = leaves * rows_b
        for s in range(leaves):
            for b in range(rows_b):
                keys[s * rows_b + b] = dests[s, 0, b] * 2 + targets[s, 0, b]

        def slot(q, carry):
            entries = [jnp.int32(blocks)] * CAP
            for block in range(blocks):
                match = keys[block] == q
                moved = [jnp.int32(block)] + entries[:-1]
                entries = [jnp.where(match, new, old) for new, old in zip(moved, entries)]
            for i in range(CAP):
                table[q * CAP + i] = entries[i]
            return carry

        lax.fori_loop(0, 2 * RING * RING, slot, 0)

    load_inv = pltpu.make_async_copy(inverses, inv_view(px, None), load.at[1])
    load_dest = pltpu.make_async_copy(dest, dests, load.at[2])
    load_target = pltpu.make_async_copy(target, targets, load.at[3])
    load_inv.start()
    load_dest.start()
    load_target.start()
    for k in range(n_chunks):
        load_pan(k).start()

    barrier = pltpu.get_barrier_semaphore()
    neighbours = (x_next, x_prev, mate, y_next, y_prev, y_far, z_next, z_prev, z_far)
    for device in neighbours:
        pl.semaphore_signal(barrier, inc=1, device_id=device, device_id_type=MESH)
    upd[upd.shape[0] - 1] = jnp.zeros(upd.shape[1:], upd.dtype)
    pl.semaphore_wait(barrier, len(neighbours))

    load_inv.wait()
    for n in (0, 1, 2):
        gather_copy(*inv_args, n).start()
    own = pan.at[:, :, :, px]
    pltpu.make_async_copy(own, own, load.at[0]).wait()
    for n in (0, 1, 2):
        gather_copy(*pan_args(0), n).start()
    load_dest.wait()
    load_target.wait()
    make_table()
    gather_wait(*inv_args, 0)
    for n in (3, 4, 5, 6):
        gather_copy(*inv_args, n).start()

    def in_turn(k, first, stage):
        @pl.when(jnp.logical_and(k >= first, k < n_chunks))
        def _():
            stage(k)

    def relay_first(k):
        gather_wait(*pan_args(k), 0)
        for n in (3, 4, 5, 6):
            gather_copy(*pan_args(k), n).start()

        if isinstance(k, int):
            for later in range(k + 1, k + 1 + AHEAD):
                for n in (0, 1, 2):
                    gather_copy(*pan_args(later), n).start()
            return

        @pl.when(k + AHEAD < n_chunks)
        def _():
            for n in (0, 1, 2):
                gather_copy(*pan_args(k + AHEAD), n).start()

    def relay_second(k):
        gather_wait(*pan_args(k), 1)
        for n in (7, 8):
            gather_copy(*pan_args(k), n).start()

    def relay_inverses():
        gather_wait(*inv_args, 1)
        for n in (7, 8):
            gather_copy(*inv_args, n).start()

    def make_factor():
        gather_wait(*inv_args, 2)

        def leaf(s, carry):
            real = pan[:, 0, s, px].reshape(width, width)
            imag = pan[:, 1, s, px].reshape(width, width)
            inv_real, inv_imag = inv[0, s], inv[1, s]
            factor[0, s] = (dot(real, inv_real) - dot(imag, inv_imag)).astype(factor.dtype)
            turned = dot(real, inv_imag) + dot(imag, inv_real)
            factor[1, s] = turned.astype(factor.dtype)
            minus[s] = (-turned).astype(minus.dtype)
            return carry

        lax.fori_loop(0, leaves, leaf, 0)

    def multiply(k):
        gather_wait(*pan_args(k), 2)

        def leaf(s, carry):
            real = pan[k, 0, s].reshape(rows_b * h, width)
            imag = pan[k, 1, s].reshape(rows_b * h, width)
            first = pl.multiple_of(s * rows_b, rows_b)
            product = dot_t(real, factor[0, s]) + dot_t(imag, minus[s])
            upd[pl.ds(first, rows_b), 0] = product.astype(upd.dtype).reshape(rows_b, h, width)
            product = dot_t(real, factor[1, s]) + dot_t(imag, factor[0, s])
            upd[pl.ds(first, rows_b), 1] = product.astype(upd.dtype).reshape(rows_b, h, width)
            return carry

        lax.fori_loop(0, leaves, leaf, 0, unroll=leaves)

        def merge(q, carry):
            half, f, g = q // 16, (q // 4) % 4, q % 4
            owner = at_yz(f + half * (g - f), g + half * (f - g))
            entry = (owner * 2 + half) * CAP
            total = upd[table[entry]].astype(jnp.float32)
            for i in range(1, CAP):
                total += upd[table[entry + i]].astype(jnp.float32)
            mer[k, half, f, g] = total.astype(mer.dtype)
            return carry

        lax.fori_loop(0, 32, merge, 0, unroll=UNROLL)
        for n in (0, 1, 2, 3):
            for half in (0, 1):
                sum_copy(k, half, n).start()

    def add_to(ref, other):
        ref[...] = (ref[...].astype(jnp.float32) + other[...].astype(jnp.float32)).astype(ref.dtype)

    def sum_b(k):
        sum_wait(k, 0)
        for half in (0, 1):
            add_to(mer.at[k, half, 1, 0:2], t1.at[k, half, 0])
            add_to(mer.at[k, half, 3, 2:4], t1.at[k, half, 1])
        for half in (0, 1):
            for n in (4, 5):
                sum_copy(k, half, n).start()

    def sum_c(k):
        sum_wait(k, 1)
        for half in (0, 1):
            total = mer[k, half, 0].astype(jnp.float32)
            total += g1[k, half, 0].astype(jnp.float32)
            total += g1[k, half, 1].astype(jnp.float32)
            mer[k, half, 0] = total.astype(mer.dtype)
        for n in (6, 7, 8):
            for half in (0, 1):
                sum_copy(k, half, n).start()

    def sum_e(k):
        sum_wait(k, 2)
        for half in (0, 1):
            total = mer[k, half, 0, 0].astype(jnp.float32)
            for n in range(3):
                total += g2[k, half, n].astype(jnp.float32)
            rows = pl.ds(pl.multiple_of(k * h, h), h)
            summed[half, :, rows] = total
        gather_drain(*pan_args(k))
        sum_drain(k)

    relay_first(0)
    relay_inverses()
    relay_second(0)
    make_factor()
    multiply(0)

    stages = {
        "1": relay_first, "2": relay_second, "m": multiply, "b": sum_b, "c": sum_c, "e": sum_e
    }

    def step(i, carry):
        for name, lag in LOOP:
            in_turn(i - lag, 1 if name in "12m" else 0, stages[name])
        return carry

    last = max(lag for _, lag in LOOP)
    lax.fori_loop(1, n_chunks + last, step, 0)

    gather_drain(*inv_args)


def finish(factor, summed, ancestors, factor_out, schur, res, out, fac_out):
    rows = summed.shape[2]
    keep = [
        pltpu.make_async_copy(factor.at[n], factor_out.at[n], fac_out.at[n]) for n in (0, 1)
    ]
    for one in keep:
        one.start()
    for t in (0, 1):
        for plane in (0, 1):
            here = pl.ds(t * rows, rows)
            res[plane, here] = ancestors[plane, here] - summed[t, plane].T
            store = pltpu.make_async_copy(
                res.at[plane, here], schur.at[plane, here], out.at[t, plane]
            )
            store.start()
            keep.append(store)
    for one in keep:
        one.wait()


def local(panels, inverses, dest, target, ancestors):
    panels = pltpu.with_memory_space_constraint(panels, pltpu.HBM)
    inverses = pltpu.with_memory_space_constraint(inverses, pltpu.HBM)
    dest = pltpu.with_memory_space_constraint(dest, pltpu.HBM)
    target = pltpu.with_memory_space_constraint(target, pltpu.HBM)
    _, leaves, rows, width = panels.shape
    rows_b = dest.shape[2]
    h = rows // CHUNKS
    blocks = leaves * rows_b
    bf16, f32 = jnp.bfloat16, jnp.float32
    any_space = pl.BlockSpec(memory_space=pl.ANY)
    vmem = pl.BlockSpec(memory_space=pltpu.VMEM)
    hbm = pl.BlockSpec(memory_space=pltpu.HBM)
    dma = pltpu.SemaphoreType.DMA
    factor, summed = pl.pallas_call(
        kernel,
        out_shape=(
            jax.ShapeDtypeStruct(panels.shape, bf16),
            jax.ShapeDtypeStruct((2, 2, rows, width), f32),
        ),
        in_specs=[hbm, hbm, hbm, hbm],
        out_specs=(vmem, vmem),
        scratch_shapes=[
            pltpu.SMEM(dest.shape, jnp.int32), pltpu.SMEM(dest.shape, jnp.int32),
            pltpu.SMEM((blocks,), jnp.int32),
            pltpu.SMEM((2 * RING * RING * CAP,), jnp.int32),
            pltpu.VMEM((CHUNKS, 2, leaves, rows_b, h, width), bf16),
            pltpu.VMEM((2, leaves, width, width), bf16),
            pltpu.VMEM((leaves, rows, width), bf16),
            pltpu.VMEM((blocks + 1, 2, h, width), bf16),
            pltpu.VMEM((CHUNKS, 2, 4, 4, 2, h, width), bf16),
            pltpu.VMEM((CHUNKS, 2, 2, 2, 2, h, width), bf16),
            pltpu.VMEM((CHUNKS, 2, 2, 4, 2, h, width), bf16),
            pltpu.VMEM((CHUNKS, 2, 3, 2, h, width), bf16),
            dma((CHUNKS,)), dma((CHUNKS, 3)), dma((1,)), dma((3,)),
            dma((CHUNKS,)), dma((CHUNKS, 3)), dma((4,)),
        ],
        compiler_params=pltpu.CompilerParams(
            collective_id=0, has_side_effects=True, vmem_limit_bytes=40 * 1024 * 1024
        ),
    )(dest, target, panels, inverses)
    return pl.pallas_call(
        finish,
        out_shape=(
            jax.ShapeDtypeStruct(panels.shape, bf16),
            jax.ShapeDtypeStruct(ancestors.shape, f32),
        ),
        in_specs=[vmem, vmem, vmem],
        out_specs=(any_space, any_space),
        scratch_shapes=[pltpu.VMEM(ancestors.shape, f32), dma((2, 2)), dma((2,))],
        compiler_params=pltpu.CompilerParams(vmem_limit_bytes=8 * 1024 * 1024),
    )(factor, summed, ancestors)


def solution(mesh):
    return jax.shard_map(
        local,
        mesh=mesh,
        in_specs=(
            P(None, "pcol", "prow", None),
            P(None, "pcol", "prow", None),
            P("pcol", "prow", None),
            P("pcol", "prow", None),
            P(None, "prow", "pcol"),
        ),
        out_specs=(P(None, "pcol", "prow", None), P(None, "prow", "pcol")),
        check_vma=False,
    )
```

```python
import functools

import jax
import jax.numpy as jnp
from jax import lax
from jax.experimental import pallas as pl
from jax.experimental.pallas import tpu as pltpu
from jax.sharding import PartitionSpec as P

MESH = pl.DeviceIdType.MESH
CHUNKS = 8
RING = 4
CAP = 6
AHEAD = 2
LOOP = (("1", 0), ("e", 4), ("c", 3), ("2", 1), ("b", 2), ("m", 1))
UNROLL = 4
WAITED = (0, 0, 2, 1, 1, 2, 2, 2, 2)


def dot(a, b):
    return jnp.dot(a, b, preferred_element_type=jnp.float32)


def dot_t(a, b):
    return lax.dot_general(a, b, (((1,), (1,)), ((), ())), preferred_element_type=jnp.float32)


def kernel(
    dest, target, panels, inverses, factor, summed,
    dests, targets, keys, table, pan, inv, minus, upd, mer, t1, g1, g2,
    psend, precv, isend, irecv, rsend, rrecv, load,
):
    n_chunks, _, leaves, rows_b, h, width = pan.shape
    part = inverses.shape[2]
    px, pc = lax.axis_index("prow"), lax.axis_index("pcol")
    x, core = px // 2, px % 2
    z, y = pc // RING, pc % RING

    def at_x(step, other=0):
        return ((x + step) % RING) * 2 + (core if not other else 1 - core)

    def at_yz(dy, dz):
        return ((z + dz) % RING) * RING + (y + dy) % RING

    x_next, x_prev, mate = (at_x(1), pc), (at_x(3), pc), (at_x(0, 1), pc)
    y_next, y_prev = (px, at_yz(1, 0)), (px, at_yz(3, 0))
    z_next, z_prev = (px, at_yz(0, 1)), (px, at_yz(0, 3))
    y_far, z_far = (px, at_yz(2, 0)), (px, at_yz(0, 2))

    def remote(src, dst, send, recv, device):
        return pltpu.make_async_remote_copy(
            src_ref=src, dst_ref=dst, send_sem=send, recv_sem=recv,
            device_id=device, device_id_type=MESH,
        )

    def gather_copy(view, send, recv, n):
        blocks = (px, px, px, at_x(3), at_x(1), at_x(3), at_x(1), at_x(2), at_x(2))
        planes = (None, None, None, 0, 1, None, None, 0, 1)
        devices = (x_next, x_prev, mate, x_next, x_prev, mate, mate, mate, mate)
        src = view(blocks[n], planes[n])
        return remote(src, src, send, recv.at[WAITED[n]], devices[n])

    def gather_wait(view, send, recv, group):
        part_of = view(0, None, (2, 1, 4)[group])
        remote(part_of, part_of, send, recv.at[group], mate).wait_recv()

    def gather_drain(view, send, recv):
        part_of = view(0, None, 7)
        remote(part_of, part_of, send, recv.at[0], mate).wait_send()

    def pan_args(k):
        def view(block, plane, count=None):
            if count:
                return pan.at[k, :, :, 0:count]
            return pan.at[k, :, :, block] if plane is None else pan.at[k, plane, :, block]

        return view, psend.at[k], precv.at[k]

    def inv_view(block, plane, count=None):
        if count:
            return inv.at[:, :, 0 : count * part]
        rows = pl.ds(pl.multiple_of(block * part, part), part)
        return inv.at[:, :, rows] if plane is None else inv.at[plane, :, rows]

    inv_args = (inv_view, isend.at[0], irecv)

    def sum_copy(k, half, n):
        along_y, along_z = (y_next, y_prev, y_far), (z_next, z_prev, z_far)
        first, then = (along_y, along_z) if half == 0 else (along_z, along_y)
        m, t, g, gg = mer.at[k, half], t1.at[k, half], g1.at[k, half], g2.at[k, half]
        src, dst, device = (
            (m.at[2, 0:2], t.at[0], first[0]),
            (m.at[2, 2:4], t.at[1], first[1]),
            (m.at[1, 2:4], g.at[0, 2:4], first[0]),
            (m.at[3, 0:2], g.at[1, 0:2], first[1]),
            (m.at[1, 0:2], g.at[0, 0:2], first[0]),
            (m.at[3, 2:4], g.at[1, 2:4], first[1]),
            (m.at[0, 2], gg.at[2], then[2]),
            (m.at[0, 1], gg.at[0], then[0]),
            (m.at[0, 3], gg.at[1], then[1]),
        )[n]
        return remote(src, dst, rsend.at[k], rrecv.at[k, (0, 0, 1, 1, 1, 1, 2, 2, 2)[n]], device)

    def sum_wait(k, group):
        part_of = upd.at[0 : (8, 16, 6)[group]]
        remote(part_of, part_of, rsend.at[k], rrecv.at[k, group], mate).wait_recv()

    def sum_drain(k):
        part_of = upd.at[0:30]
        remote(part_of, part_of, rsend.at[k], rrecv.at[k, 0], mate).wait_send()

    def load_pan(k):
        rows = pl.ds(pl.multiple_of(k * h, h), h)
        return pltpu.make_async_copy(panels.at[:, :, rows], pan.at[k, :, :, px], load.at[0])

    def make_table():
        blocks = leaves * rows_b
        for s in range(leaves):
            for b in range(rows_b):
                keys[s * rows_b + b] = dests[s, 0, b] * 2 + targets[s, 0, b]

        def slot(q, carry):
            entries = [jnp.int32(blocks)] * CAP
            for block in range(blocks):
                match = keys[block] == q
                moved = [jnp.int32(block)] + entries[:-1]
                entries = [jnp.where(match, new, old) for new, old in zip(moved, entries)]
            for i in range(CAP):
                table[q * CAP + i] = entries[i]
            return carry

        lax.fori_loop(0, 2 * RING * RING, slot, 0)

    load_inv = pltpu.make_async_copy(inverses, inv_view(px, None), load.at[1])
    load_dest = pltpu.make_async_copy(dest, dests, load.at[2])
    load_target = pltpu.make_async_copy(target, targets, load.at[3])
    load_inv.start()
    load_dest.start()
    load_target.start()
    for k in range(n_chunks):
        load_pan(k).start()

    barrier = pltpu.get_barrier_semaphore()
    neighbours = (x_next, x_prev, mate, y_next, y_prev, y_far, z_next, z_prev, z_far)
    for device in neighbours:
        pl.semaphore_signal(barrier, inc=1, device_id=device, device_id_type=MESH)
    upd[upd.shape[0] - 1] = jnp.zeros(upd.shape[1:], upd.dtype)
    pl.semaphore_wait(barrier, len(neighbours))

    load_inv.wait()
    for n in (0, 1, 2):
        gather_copy(*inv_args, n).start()
    own = pan.at[:, :, :, px]
    pltpu.make_async_copy(own, own, load.at[0]).wait()
    for n in (0, 1, 2):
        gather_copy(*pan_args(0), n).start()
    load_dest.wait()
    load_target.wait()
    make_table()
    gather_wait(*inv_args, 0)
    for n in (3, 4, 5, 6):
        gather_copy(*inv_args, n).start()

    def in_turn(k, first, stage):
        @pl.when(jnp.logical_and(k >= first, k < n_chunks))
        def _():
            stage(k)

    def relay_first(k):
        gather_wait(*pan_args(k), 0)
        for n in (3, 4, 5, 6):
            gather_copy(*pan_args(k), n).start()

        if isinstance(k, int):
            for later in range(k + 1, k + 1 + AHEAD):
                for n in (0, 1, 2):
                    gather_copy(*pan_args(later), n).start()
            return

        @pl.when(k + AHEAD < n_chunks)
        def _():
            for n in (0, 1, 2):
                gather_copy(*pan_args(k + AHEAD), n).start()

    def relay_second(k):
        gather_wait(*pan_args(k), 1)
        for n in (7, 8):
            gather_copy(*pan_args(k), n).start()

    def relay_inverses():
        gather_wait(*inv_args, 1)
        for n in (7, 8):
            gather_copy(*inv_args, n).start()

    def make_factor():
        gather_wait(*inv_args, 2)

        def leaf(s, carry):
            real = pan[:, 0, s, px].reshape(width, width)
            imag = pan[:, 1, s, px].reshape(width, width)
            inv_real, inv_imag = inv[0, s], inv[1, s]
            factor[0, s] = (dot(real, inv_real) - dot(imag, inv_imag)).astype(factor.dtype)
            turned = dot(real, inv_imag) + dot(imag, inv_real)
            factor[1, s] = turned.astype(factor.dtype)
            minus[s] = (-turned).astype(minus.dtype)
            return carry

        lax.fori_loop(0, leaves, leaf, 0)

    def multiply(k):
        gather_wait(*pan_args(k), 2)

        def leaf(s, carry):
            real = pan[k, 0, s].reshape(rows_b * h, width)
            imag = pan[k, 1, s].reshape(rows_b * h, width)
            first = pl.multiple_of(s * rows_b, rows_b)
            product = dot_t(real, factor[0, s]) + dot_t(imag, minus[s])
            upd[pl.ds(first, rows_b), 0] = product.astype(upd.dtype).reshape(rows_b, h, width)
            product = dot_t(real, factor[1, s]) + dot_t(imag, factor[0, s])
            upd[pl.ds(first, rows_b), 1] = product.astype(upd.dtype).reshape(rows_b, h, width)
            return carry

        lax.fori_loop(0, leaves, leaf, 0, unroll=leaves)

        def merge(half, f, g):
            owner = at_yz(f + half * (g - f), g + half * (f - g))
            entry = (owner * 2 + half) * CAP
            total = upd[table[entry]].astype(jnp.float32)
            for i in range(1, CAP):
                total += upd[table[entry + i]].astype(jnp.float32)
            mer[k, half, f, g] = total.astype(mer.dtype)

        def farthest(q, carry):
            merge(q // 4, 2, q % 4)
            return carry

        def beside(q, carry):
            merge(q // 8, 1 + 2 * ((q // 4) % 2), q % 4)
            return carry

        def own(q, carry):
            merge(q // 4, 0, q % 4)
            return carry

        lax.fori_loop(0, 8, farthest, 0, unroll=UNROLL)
        for n in (0, 1):
            for half in (0, 1):
                sum_copy(k, half, n).start()
        lax.fori_loop(0, 16, beside, 0, unroll=UNROLL)
        for n in (2, 3):
            for half in (0, 1):
                sum_copy(k, half, n).start()
        lax.fori_loop(0, 8, own, 0, unroll=UNROLL)

    def add_to(ref, other):
        ref[...] = (ref[...].astype(jnp.float32) + other[...].astype(jnp.float32)).astype(ref.dtype)

    def sum_b(k):
        sum_wait(k, 0)
        for half in (0, 1):
            add_to(mer.at[k, half, 1, 0:2], t1.at[k, half, 0])
            add_to(mer.at[k, half, 3, 2:4], t1.at[k, half, 1])
        for half in (0, 1):
            for n in (4, 5):
                sum_copy(k, half, n).start()

    def sum_c(k):
        sum_wait(k, 1)
        for half in (0, 1):
            total = mer[k, half, 0].astype(jnp.float32)
            total += g1[k, half, 0].astype(jnp.float32)
            total += g1[k, half, 1].astype(jnp.float32)
            mer[k, half, 0] = total.astype(mer.dtype)
        for n in (6, 7, 8):
            for half in (0, 1):
                sum_copy(k, half, n).start()

    def sum_e(k):
        sum_wait(k, 2)
        for half in (0, 1):
            total = mer[k, half, 0, 0].astype(jnp.float32)
            for n in range(3):
                total += g2[k, half, n].astype(jnp.float32)
            rows = pl.ds(pl.multiple_of(k * h, h), h)
            summed[half, :, rows] = total
        gather_drain(*pan_args(k))
        sum_drain(k)

    relay_first(0)
    relay_inverses()
    relay_second(0)
    make_factor()
    multiply(0)

    stages = {
        "1": relay_first, "2": relay_second, "m": multiply, "b": sum_b, "c": sum_c, "e": sum_e
    }

    def step(i, carry):
        for name, lag in LOOP:
            in_turn(i - lag, 1 if name in "12m" else 0, stages[name])
        return carry

    last = max(lag for _, lag in LOOP)
    lax.fori_loop(1, n_chunks + last, step, 0)

    gather_drain(*inv_args)


def finish(factor, summed, ancestors, factor_out, schur, res, out, fac_out):
    rows = summed.shape[2]
    keep = [
        pltpu.make_async_copy(factor.at[n], factor_out.at[n], fac_out.at[n]) for n in (0, 1)
    ]
    for one in keep:
        one.start()
    for t in (0, 1):
        for plane in (0, 1):
            here = pl.ds(t * rows, rows)
            res[plane, here] = ancestors[plane, here] - summed[t, plane].T
            store = pltpu.make_async_copy(
                res.at[plane, here], schur.at[plane, here], out.at[t, plane]
            )
            store.start()
            keep.append(store)
    for one in keep:
        one.wait()


def local(panels, inverses, dest, target, ancestors):
    panels = pltpu.with_memory_space_constraint(panels, pltpu.HBM)
    inverses = pltpu.with_memory_space_constraint(inverses, pltpu.HBM)
    dest = pltpu.with_memory_space_constraint(dest, pltpu.HBM)
    target = pltpu.with_memory_space_constraint(target, pltpu.HBM)
    _, leaves, rows, width = panels.shape
    rows_b = dest.shape[2]
    h = rows // CHUNKS
    blocks = leaves * rows_b
    bf16, f32 = jnp.bfloat16, jnp.float32
    any_space = pl.BlockSpec(memory_space=pl.ANY)
    vmem = pl.BlockSpec(memory_space=pltpu.VMEM)
    hbm = pl.BlockSpec(memory_space=pltpu.HBM)
    dma = pltpu.SemaphoreType.DMA
    factor, summed = pl.pallas_call(
        kernel,
        out_shape=(
            jax.ShapeDtypeStruct(panels.shape, bf16),
            jax.ShapeDtypeStruct((2, 2, rows, width), f32),
        ),
        in_specs=[hbm, hbm, hbm, hbm],
        out_specs=(vmem, vmem),
        scratch_shapes=[
            pltpu.SMEM(dest.shape, jnp.int32), pltpu.SMEM(dest.shape, jnp.int32),
            pltpu.SMEM((blocks,), jnp.int32),
            pltpu.SMEM((2 * RING * RING * CAP,), jnp.int32),
            pltpu.VMEM((CHUNKS, 2, leaves, rows_b, h, width), bf16),
            pltpu.VMEM((2, leaves, width, width), bf16),
            pltpu.VMEM((leaves, rows, width), bf16),
            pltpu.VMEM((blocks + 1, 2, h, width), bf16),
            pltpu.VMEM((CHUNKS, 2, 4, 4, 2, h, width), bf16),
            pltpu.VMEM((CHUNKS, 2, 2, 2, 2, h, width), bf16),
            pltpu.VMEM((CHUNKS, 2, 2, 4, 2, h, width), bf16),
            pltpu.VMEM((CHUNKS, 2, 3, 2, h, width), bf16),
            dma((CHUNKS,)), dma((CHUNKS, 3)), dma((1,)), dma((3,)),
            dma((CHUNKS,)), dma((CHUNKS, 3)), dma((4,)),
        ],
        compiler_params=pltpu.CompilerParams(
            collective_id=0, has_side_effects=True, vmem_limit_bytes=40 * 1024 * 1024
        ),
    )(dest, target, panels, inverses)
    return pl.pallas_call(
        finish,
        out_shape=(
            jax.ShapeDtypeStruct(panels.shape, bf16),
            jax.ShapeDtypeStruct(ancestors.shape, f32),
        ),
        in_specs=[vmem, vmem, vmem],
        out_specs=(any_space, any_space),
        scratch_shapes=[pltpu.VMEM(ancestors.shape, f32), dma((2, 2)), dma((2,))],
        compiler_params=pltpu.CompilerParams(vmem_limit_bytes=8 * 1024 * 1024),
    )(factor, summed, ancestors)


def solution(mesh):
    return jax.shard_map(
        local,
        mesh=mesh,
        in_specs=(
            P(None, "pcol", "prow", None),
            P(None, "pcol", "prow", None),
            P("pcol", "prow", None),
            P("pcol", "prow", None),
            P(None, "prow", "pcol"),
        ),
        out_specs=(P(None, "pcol", "prow", None), P(None, "prow", "pcol")),
        check_vma=False,
    )
```

```python
import functools

import jax
import jax.numpy as jnp
from jax import lax
from jax.experimental import pallas as pl
from jax.experimental.pallas import tpu as pltpu
from jax.sharding import PartitionSpec as P

MESH = pl.DeviceIdType.MESH
CHUNKS = 8
RING = 4
CAP = 6
AHEAD = 2
LOOP = (("1", 0), ("e", 4), ("c", 3), ("2", 1), ("b", 2), ("m", 1))
UNROLL = 4
WAITED = (0, 0, 2, 1, 1, 2, 2, 2, 2)


def dot(a, b):
    return jnp.dot(a, b, preferred_element_type=jnp.float32)


def dot_t(a, b):
    return lax.dot_general(a, b, (((1,), (1,)), ((), ())), preferred_element_type=jnp.float32)


def kernel(
    dest, target, panels, inverses, factor, summed,
    dests, targets, keys, table, pan, inv, minus, upd, mer, t1, g1, g2,
    psend, precv, isend, irecv, rsend, rrecv, load,
):
    n_chunks, _, leaves, rows_b, h, width = pan.shape
    part = inverses.shape[2]
    px, pc = lax.axis_index("prow"), lax.axis_index("pcol")
    x, core = px // 2, px % 2
    z, y = pc // RING, pc % RING

    def at_x(step, other=0):
        return ((x + step) % RING) * 2 + (core if not other else 1 - core)

    def at_yz(dy, dz):
        return ((z + dz) % RING) * RING + (y + dy) % RING

    x_next, x_prev, mate = (at_x(1), pc), (at_x(3), pc), (at_x(0, 1), pc)
    y_next, y_prev = (px, at_yz(1, 0)), (px, at_yz(3, 0))
    z_next, z_prev = (px, at_yz(0, 1)), (px, at_yz(0, 3))
    y_far, z_far = (px, at_yz(2, 0)), (px, at_yz(0, 2))

    def remote(src, dst, send, recv, device):
        return pltpu.make_async_remote_copy(
            src_ref=src, dst_ref=dst, send_sem=send, recv_sem=recv,
            device_id=device, device_id_type=MESH,
        )

    def gather_copy(view, send, recv, n):
        blocks = (px, px, px, at_x(3), at_x(1), at_x(3), at_x(1), at_x(2), at_x(2))
        planes = (None, None, None, 0, 1, None, None, 0, 1)
        devices = (x_next, x_prev, mate, x_next, x_prev, mate, mate, mate, mate)
        src = view(blocks[n], planes[n])
        return remote(src, src, send, recv.at[WAITED[n]], devices[n])

    def gather_wait(view, send, recv, group):
        part_of = view(0, None, (2, 1, 4)[group])
        remote(part_of, part_of, send, recv.at[group], mate).wait_recv()

    def gather_drain(view, send, recv):
        part_of = view(0, None, 7)
        remote(part_of, part_of, send, recv.at[0], mate).wait_send()

    def pan_args(k):
        def view(block, plane, count=None):
            if count:
                return pan.at[k, :, :, 0:count]
            return pan.at[k, :, :, block] if plane is None else pan.at[k, plane, :, block]

        return view, psend.at[k], precv.at[k]

    def inv_view(block, plane, count=None):
        if count:
            return inv.at[:, :, 0 : count * part]
        rows = pl.ds(pl.multiple_of(block * part, part), part)
        return inv.at[:, :, rows] if plane is None else inv.at[plane, :, rows]

    inv_args = (inv_view, isend.at[0], irecv)

    def sum_copy(k, half, n):
        along_y, along_z = (y_next, y_prev, y_far), (z_next, z_prev, z_far)
        first, then = (along_y, along_z) if half == 0 else (along_z, along_y)
        m, t, g, gg = mer.at[k, half], t1.at[k, half], g1.at[k, half], g2.at[k, half]
        src, dst, device = (
            (m.at[2, 0:2], t.at[0], first[0]),
            (m.at[2, 2:4], t.at[1], first[1]),
            (m.at[1, 2:4], g.at[0, 2:4], first[0]),
            (m.at[3, 0:2], g.at[1, 0:2], first[1]),
            (m.at[1, 0:2], g.at[0, 0:2], first[0]),
            (m.at[3, 2:4], g.at[1, 2:4], first[1]),
            (m.at[0, 2], gg.at[2], then[2]),
            (m.at[0, 1], gg.at[0], then[0]),
            (m.at[0, 3], gg.at[1], then[1]),
        )[n]
        return remote(src, dst, rsend.at[k], rrecv.at[k, (0, 0, 1, 1, 1, 1, 2, 2, 2)[n]], device)

    def sum_wait(k, group):
        part_of = upd.at[0 : (8, 16, 6)[group]]
        remote(part_of, part_of, rsend.at[k], rrecv.at[k, group], mate).wait_recv()

    def sum_drain(k):
        part_of = upd.at[0:30]
        remote(part_of, part_of, rsend.at[k], rrecv.at[k, 0], mate).wait_send()

    def load_pan(k):
        rows = pl.ds(pl.multiple_of(k * h, h), h)
        return pltpu.make_async_copy(panels.at[:, :, rows], pan.at[k, :, :, px], load.at[0])

    def make_table():
        blocks = leaves * rows_b
        for s in range(leaves):
            for b in range(rows_b):
                keys[s * rows_b + b] = dests[s, 0, b] * 2 + targets[s, 0, b]

        def slot(q, carry):
            entries = [jnp.int32(blocks)] * CAP
            for block in range(blocks):
                match = keys[block] == q
                moved = [jnp.int32(block)] + entries[:-1]
                entries = [jnp.where(match, new, old) for new, old in zip(moved, entries)]
            for i in range(CAP):
                table[q * CAP + i] = entries[i]
            return carry

        lax.fori_loop(0, 2 * RING * RING, slot, 0)

    load_inv = pltpu.make_async_copy(inverses, inv_view(px, None), load.at[1])
    load_dest = pltpu.make_async_copy(dest, dests, load.at[2])
    load_target = pltpu.make_async_copy(target, targets, load.at[3])
    load_inv.start()
    load_dest.start()
    load_target.start()
    for k in range(n_chunks):
        load_pan(k).start()

    barrier = pltpu.get_barrier_semaphore()
    neighbours = (x_next, x_prev, mate, y_next, y_prev, y_far, z_next, z_prev, z_far)
    for device in neighbours:
        pl.semaphore_signal(barrier, inc=1, device_id=device, device_id_type=MESH)
    upd[upd.shape[0] - 1] = jnp.zeros(upd.shape[1:], upd.dtype)
    pl.semaphore_wait(barrier, len(neighbours))

    load_inv.wait()
    for n in (0, 1, 2):
        gather_copy(*inv_args, n).start()
    own = pan.at[:, :, :, px]
    pltpu.make_async_copy(own, own, load.at[0]).wait()
    for n in (0, 1, 2):
        gather_copy(*pan_args(0), n).start()
    load_dest.wait()
    load_target.wait()
    make_table()
    gather_wait(*inv_args, 0)
    for n in (3, 4, 5, 6):
        gather_copy(*inv_args, n).start()

    def in_turn(k, first, stage):
        @pl.when(jnp.logical_and(k >= first, k < n_chunks))
        def _():
            stage(k)

    def relay_first(k):
        gather_wait(*pan_args(k), 0)
        for n in (3, 4, 5, 6):
            gather_copy(*pan_args(k), n).start()

        if isinstance(k, int):
            for later in range(k + 1, k + 1 + AHEAD):
                for n in (0, 1, 2):
                    gather_copy(*pan_args(later), n).start()
            return

        @pl.when(k + AHEAD < n_chunks)
        def _():
            for n in (0, 1, 2):
                gather_copy(*pan_args(k + AHEAD), n).start()

    def relay_second(k):
        gather_wait(*pan_args(k), 1)
        for n in (7, 8):
            gather_copy(*pan_args(k), n).start()

    def relay_inverses():
        gather_wait(*inv_args, 1)
        for n in (7, 8):
            gather_copy(*inv_args, n).start()

    def make_factor():
        gather_wait(*inv_args, 2)

        def leaf(s, carry):
            real = pan[:, 0, s, px].reshape(width, width)
            imag = pan[:, 1, s, px].reshape(width, width)
            inv_real, inv_imag = inv[0, s], inv[1, s]
            factor[0, s] = (dot(real, inv_real) - dot(imag, inv_imag)).astype(factor.dtype)
            turned = dot(real, inv_imag) + dot(imag, inv_real)
            factor[1, s] = turned.astype(factor.dtype)
            minus[s] = (-turned).astype(minus.dtype)
            return carry

        lax.fori_loop(0, leaves, leaf, 0)

    def multiply(k):
        gather_wait(*pan_args(k), 2)

        def leaf(s, carry):
            real = pan[k, 0, s].reshape(rows_b * h, width)
            imag = pan[k, 1, s].reshape(rows_b * h, width)
            first = pl.multiple_of(s * rows_b, rows_b)
            product = dot_t(real, factor[0, s]) + dot_t(imag, minus[s])
            upd[pl.ds(first, rows_b), 0] = product.astype(upd.dtype).reshape(rows_b, h, width)
            product = dot_t(real, factor[1, s]) + dot_t(imag, factor[0, s])
            upd[pl.ds(first, rows_b), 1] = product.astype(upd.dtype).reshape(rows_b, h, width)
            return carry

        lax.fori_loop(0, leaves, leaf, 0, unroll=leaves)

        def merge(half, f, g):
            owner = at_yz(f + half * (g - f), g + half * (f - g))
            entry = (owner * 2 + half) * CAP
            total = upd[table[entry]].astype(jnp.float32)
            for i in range(1, CAP):
                total += upd[table[entry + i]].astype(jnp.float32)
            mer[k, half, f, g] = total.astype(mer.dtype)

        def farthest(q, carry):
            merge(q // 4, 2, q % 4)
            return carry

        def beside(q, carry):
            merge(q // 8, 1 + 2 * ((q // 4) % 2), q % 4)
            return carry

        def own(q, carry):
            merge(q // 4, 0, q % 4)
            return carry

        lax.fori_loop(0, 8, farthest, 0, unroll=UNROLL)
        for n in (0, 1):
            for half in (0, 1):
                sum_copy(k, half, n).start()
        lax.fori_loop(0, 16, beside, 0, unroll=UNROLL)
        for n in (2, 3):
            for half in (0, 1):
                sum_copy(k, half, n).start()
        lax.fori_loop(0, 8, own, 0, unroll=UNROLL)

    def add_to(ref, other):
        ref[...] = (ref[...].astype(jnp.float32) + other[...].astype(jnp.float32)).astype(ref.dtype)

    def sum_b(k):
        sum_wait(k, 0)
        for half in (0, 1):
            add_to(mer.at[k, half, 1, 0:2], t1.at[k, half, 0])
            add_to(mer.at[k, half, 3, 2:4], t1.at[k, half, 1])
        for half in (0, 1):
            for n in (4, 5):
                sum_copy(k, half, n).start()

    def sum_c(k):
        sum_wait(k, 1)
        for g, ready in ((2, None), (1, 6), (3, 7), (0, 8)):
            for half in (0, 1):
                total = mer[k, half, 0, g].astype(jnp.float32)
                total += g1[k, half, 0, g].astype(jnp.float32)
                total += g1[k, half, 1, g].astype(jnp.float32)
                mer[k, half, 0, g] = total.astype(mer.dtype)
            if ready:
                for half in (0, 1):
                    sum_copy(k, half, ready).start()

    def sum_e(k):
        sum_wait(k, 2)
        for half in (0, 1):
            total = mer[k, half, 0, 0].astype(jnp.float32)
            for n in range(3):
                total += g2[k, half, n].astype(jnp.float32)
            rows = pl.ds(pl.multiple_of(k * h, h), h)
            summed[half, :, rows] = total
        gather_drain(*pan_args(k))
        sum_drain(k)

    relay_first(0)
    relay_inverses()
    relay_second(0)
    make_factor()
    multiply(0)

    stages = {
        "1": relay_first, "2": relay_second, "m": multiply, "b": sum_b, "c": sum_c, "e": sum_e
    }

    def step(i, carry):
        for name, lag in LOOP:
            in_turn(i - lag, 1 if name in "12m" else 0, stages[name])
        return carry

    last = max(lag for _, lag in LOOP)
    lax.fori_loop(1, n_chunks + last, step, 0)

    gather_drain(*inv_args)


def finish(factor, summed, ancestors, factor_out, schur, res, out, fac_out):
    rows = summed.shape[2]
    keep = [
        pltpu.make_async_copy(factor.at[n], factor_out.at[n], fac_out.at[n]) for n in (0, 1)
    ]
    for one in keep:
        one.start()
    for t in (0, 1):
        for plane in (0, 1):
            here = pl.ds(t * rows, rows)
            res[plane, here] = ancestors[plane, here] - summed[t, plane].T
            store = pltpu.make_async_copy(
                res.at[plane, here], schur.at[plane, here], out.at[t, plane]
            )
            store.start()
            keep.append(store)
    for one in keep:
        one.wait()


def local(panels, inverses, dest, target, ancestors):
    panels = pltpu.with_memory_space_constraint(panels, pltpu.HBM)
    inverses = pltpu.with_memory_space_constraint(inverses, pltpu.HBM)
    dest = pltpu.with_memory_space_constraint(dest, pltpu.HBM)
    target = pltpu.with_memory_space_constraint(target, pltpu.HBM)
    _, leaves, rows, width = panels.shape
    rows_b = dest.shape[2]
    h = rows // CHUNKS
    blocks = leaves * rows_b
    bf16, f32 = jnp.bfloat16, jnp.float32
    any_space = pl.BlockSpec(memory_space=pl.ANY)
    vmem = pl.BlockSpec(memory_space=pltpu.VMEM)
    hbm = pl.BlockSpec(memory_space=pltpu.HBM)
    dma = pltpu.SemaphoreType.DMA
    factor, summed = pl.pallas_call(
        kernel,
        out_shape=(
            jax.ShapeDtypeStruct(panels.shape, bf16),
            jax.ShapeDtypeStruct((2, 2, rows, width), f32),
        ),
        in_specs=[hbm, hbm, hbm, hbm],
        out_specs=(vmem, vmem),
        scratch_shapes=[
            pltpu.SMEM(dest.shape, jnp.int32), pltpu.SMEM(dest.shape, jnp.int32),
            pltpu.SMEM((blocks,), jnp.int32),
            pltpu.SMEM((2 * RING * RING * CAP,), jnp.int32),
            pltpu.VMEM((CHUNKS, 2, leaves, rows_b, h, width), bf16),
            pltpu.VMEM((2, leaves, width, width), bf16),
            pltpu.VMEM((leaves, rows, width), bf16),
            pltpu.VMEM((blocks + 1, 2, h, width), bf16),
            pltpu.VMEM((CHUNKS, 2, 4, 4, 2, h, width), bf16),
            pltpu.VMEM((CHUNKS, 2, 2, 2, 2, h, width), bf16),
            pltpu.VMEM((CHUNKS, 2, 2, 4, 2, h, width), bf16),
            pltpu.VMEM((CHUNKS, 2, 3, 2, h, width), bf16),
            dma((CHUNKS,)), dma((CHUNKS, 3)), dma((1,)), dma((3,)),
            dma((CHUNKS,)), dma((CHUNKS, 3)), dma((4,)),
        ],
        compiler_params=pltpu.CompilerParams(
            collective_id=0, has_side_effects=True, vmem_limit_bytes=40 * 1024 * 1024
        ),
    )(dest, target, panels, inverses)
    return pl.pallas_call(
        finish,
        out_shape=(
            jax.ShapeDtypeStruct(panels.shape, bf16),
            jax.ShapeDtypeStruct(ancestors.shape, f32),
        ),
        in_specs=[vmem, vmem, vmem],
        out_specs=(any_space, any_space),
        scratch_shapes=[pltpu.VMEM(ancestors.shape, f32), dma((2, 2)), dma((2,))],
        compiler_params=pltpu.CompilerParams(vmem_limit_bytes=8 * 1024 * 1024),
    )(factor, summed, ancestors)


def solution(mesh):
    return jax.shard_map(
        local,
        mesh=mesh,
        in_specs=(
            P(None, "pcol", "prow", None),
            P(None, "pcol", "prow", None),
            P("pcol", "prow", None),
            P("pcol", "prow", None),
            P(None, "prow", "pcol"),
        ),
        out_specs=(P(None, "pcol", "prow", None), P(None, "prow", "pcol")),
        check_vma=False,
    )
```
